256 devices in a mesh: px: 2 (over core), py: 8 (over z), ta: 16 (over y, x).
Axes of the slice: x: 4, y: 4, z: 8, core: 2. Of those that a mesh axis runs over, the one named last changes fastest.
Arguments:
- snapshots: bfloat16 [384, 5, 131072], P('ta', None, ('px', 'py')), may hold values from -6 to 6
- quad_weights: float32 [131072], P(('px', 'py')), may hold values from 1 to 10
- spectral_indices: int32 [32], replicated, may hold values from 0 to 127
Outputs:
- spectra: float32 [32, 2, 2, 5, 131072], P('ta', None, None, None, ('px', 'py'))
- gram: float32 [32, 2, 2, 2], P('ta')
The draws below stay inside these ranges and needn't reach their ends.
All inputs are finite; a program needn't handle non-finite values.
Results may differ from the reference program's by a relative error of at most 0.0042.
Values may be sent and summed in bfloat16 or wider, within the bound.
No kernel may reach another device: no remote copies, remote signals or barrier semaphores. Data moves between devices by JAX's collectives and lax.ppermute only.
A program may use at most 128 MiB of HBM per device.

```python
import math
import jax
import jax.numpy as jnp
from jax import lax

VARS = 5
BLK = 256
HOP = 128
SEGMENT_NUMBER = 2
RECORD_LENGTH = 384
RETAINED_MODES = 32
POINTS = 131072


def place_ends(values, key, least, high):
    index_at = [jax.random.randint(jax.random.fold_in(key, axis), (), 0, length) for axis, length in enumerate(values.shape)]
    widest = values.shape.index(max(values.shape))
    beside = index_at[:widest] + [(index_at[widest] + 1) % values.shape[widest]] + index_at[widest + 1:]
    return values.at[tuple(index_at)].set(least).at[tuple(beside)].set(high)


def block_levels(key, dims, cuts, low, top_value):
    def one(axis_at, parts):
        draws = jax.random.uniform(jax.random.fold_in(jax.random.fold_in(key, 6), axis_at), (parts,), jnp.float32, low / len(cuts), top_value / len(cuts))
        return jnp.repeat(jnp.exp(draws), dims[axis_at] // parts).reshape((-1,) + (1,) * (len(dims) - axis_at - 1))

    loudness = one(*cuts[0])
    for cut in cuts[1:]:
        loudness = loudness * one(*cut)
    return loudness


def scatter_about(rng, dims, spread, most, pieces=(), kind=jnp.bfloat16):
    loudness = block_levels(rng, dims, pieces, -0.22, 0.18) if pieces else 1.0
    entries = jax.random.normal(rng, dims, jnp.float32) * spread * loudness
    return jnp.minimum(jnp.maximum(entries, -most), most).astype(kind)


def setup_inputs(seed: int = 0) -> dict:
    key_list = jax.random.split(jax.random.key(seed), 4)
    return {
        "snapshots": scatter_about(key_list[0], (RECORD_LENGTH, VARS, POINTS), 1.0, 6.0, ((0, 16), (2, 16))),
        "quad_weights": jnp.clip(jnp.exp(math.log(10.0) - 2.3025851 * jax.random.uniform(key_list[1], (POINTS,), jnp.float32) ** block_levels(key_list[1], (POINTS,), ((0, 16),), -0.2, 0.2)), 1.0, 10.0),
        "spectral_indices": place_ends(jax.random.randint(key_list[2], (RETAINED_MODES,), 0, BLK // 2), jax.random.fold_in(key_list[2], 1), 0, (BLK // 2) - 1).astype(jnp.int32),
    }


def make_rotation_multipliers(spectral_indices, temporal_locations):
    segment_beginnings = jnp.arange(SEGMENT_NUMBER, dtype=jnp.int32) * HOP
    segment_shifts = temporal_locations[None, :] - segment_beginnings[:, None]
    inside = (segment_shifts >= 0) & (segment_shifts < BLK)
    window = 0.5 - 0.5 * jnp.cos(2.0 * math.pi * segment_shifts.astype(jnp.float32) / BLK)
    window = jnp.where(inside, window, jnp.float32(0.0)) / jnp.sqrt(jnp.float32(3.0 * BLK / 8.0))
    phases = jnp.mod(spectral_indices[:, None, None] * segment_shifts[None, :, :], BLK)
    angles = 2.0 * math.pi * phases.astype(jnp.float32) / BLK
    real_part = jnp.cos(angles) * window[None]
    imag_part = -jnp.sin(angles) * window[None]
    gathered_segments = jnp.stack([real_part, imag_part], axis=2)
    return gathered_segments.reshape(RETAINED_MODES * SEGMENT_NUMBER * 2, temporal_locations.shape[0]).astype(jnp.bfloat16)

def gram_terms(spectra):
    flat = spectra.reshape(spectra.shape[0], 2 * SEGMENT_NUMBER, -1)
    inner = jnp.einsum('fam,fbm->fab', flat, flat, precision=lax.Precision.HIGHEST)
    inner = inner.reshape(spectra.shape[0], SEGMENT_NUMBER, 2, SEGMENT_NUMBER, 2)
    real_part = inner[:, :, 0, :, 0] + inner[:, :, 1, :, 1]
    imag_part = inner[:, :, 0, :, 1] - inner[:, :, 1, :, 0]
    return jnp.stack([real_part, imag_part], axis=-1)

def reference(snapshots, quad_weights, spectral_indices):
    temporal_locations = jnp.arange(RECORD_LENGTH, dtype=jnp.int32)
    rotation_multipliers = make_rotation_multipliers(spectral_indices, temporal_locations)
    flat_snapshots = snapshots.reshape(RECORD_LENGTH, VARS * POINTS)
    raw = jnp.dot(rotation_multipliers, flat_snapshots, preferred_element_type=jnp.float32)
    raw = raw.reshape(RETAINED_MODES, SEGMENT_NUMBER, 2, VARS, POINTS)
    spectra = raw * jnp.sqrt(quad_weights)
    gram = gram_terms(spectra) / jnp.float32(POINTS * VARS)
    return (spectra, gram)
```

```python
import math

import jax
import jax.numpy as jnp
from jax import lax
from jax.experimental import pallas as pl
from jax.experimental.pallas import tpu as pltpu
from jax.sharding import PartitionSpec as P

VARS = 5
BLK = 256
HOP = 128
SEGMENT_NUMBER = 2
RECORD_LENGTH = 384
RETAINED_MODES = 32
LANES = 128


def make_rotation_multipliers(spectral_indices, temporal_locations):
    segment_beginnings = jnp.arange(SEGMENT_NUMBER, dtype=jnp.int32) * HOP
    segment_shifts = temporal_locations[None, :] - segment_beginnings[:, None]
    inside = (segment_shifts >= 0) & (segment_shifts < BLK)
    window = 0.5 - 0.5 * jnp.cos(2.0 * math.pi * segment_shifts.astype(jnp.float32) / BLK)
    window = jnp.where(inside, window, jnp.float32(0.0)) / jnp.sqrt(jnp.float32(3.0 * BLK / 8.0))
    phases = jnp.mod(spectral_indices[None, :, None] * segment_shifts[:, None, :], BLK)
    angles = 2.0 * math.pi * phases.astype(jnp.float32) / BLK
    real_part = jnp.cos(angles) * window[:, None]
    imag_part = -jnp.sin(angles) * window[:, None]
    return (
        jnp.stack([real_part, imag_part], axis=0)
        .reshape(2 * SEGMENT_NUMBER * RETAINED_MODES, temporal_locations.shape[0])
        .astype(jnp.bfloat16)
    )


def pack(shard, groups):
    variables, times, points = shard.shape
    piece = points // groups
    per_step = 4

    def body(x_ref, o_ref):
        for d in range(per_step):
            o_ref[d] = x_ref[:, :, d * piece : (d + 1) * piece]

    return pl.pallas_call(
        body,
        grid=(groups // per_step,),
        in_specs=[pl.BlockSpec((variables, times, per_step * piece), lambda j: (0, 0, j))],
        out_specs=pl.BlockSpec((per_step, variables, times, piece), lambda j: (j, 0, 0, 0)),
        out_shape=jax.ShapeDtypeStruct((groups, variables, times, piece), shard.dtype),
        name="pack",
    )(shard)


def transform(gathered, multipliers, weights, group):
    groups, variables, times, piece = gathered.shape
    rows = multipliers.shape[0]
    tiles = piece // LANES
    modes = RETAINED_MODES
    per_mode = SEGMENT_NUMBER * variables * tiles * 2

    def body(g_ref, x_ref, m_ref, w_ref, z_ref, gram_ref, f_ref, acc_ref):
        m = m_ref[...]
        acc_ref[...] = jnp.zeros_like(acc_ref)
        sw = jnp.sqrt(w_ref[pl.ds(g_ref[0] * tiles, tiles), :])
        for v in range(variables):
            x = x_ref[:, v].reshape(groups * times, piece)
            s = jnp.dot(m, x, preferred_element_type=jnp.float32)
            for j in range(tiles):
                q = s[:, j * LANES : (j + 1) * LANES] * sw[j : j + 1, :]
                parts = {}
                for c in range(2):
                    for b in range(SEGMENT_NUMBER):
                        at = (c * SEGMENT_NUMBER + b) * modes
                        part = q[at : at + modes]
                        parts[c, b] = part
                        first = (b * variables + v) * tiles * 2 + j * 2 + c
                        f_ref[pl.ds(first, modes, stride=per_mode), :] = part
                r0, r1, i0, i1 = parts[0, 0], parts[0, 1], parts[1, 0], parts[1, 1]
                acc_ref[0:modes] += r0 * r0 + i0 * i0
                acc_ref[modes : 2 * modes] += r1 * r1 + i1 * i1
                acc_ref[2 * modes : 3 * modes] += r0 * r1 + i0 * i1
                acc_ref[3 * modes : 4 * modes] += r0 * i1 - i0 * r1
        z_ref[...] = f_ref[...].astype(z_ref.dtype)
        gram_ref[...] = lax.dot_general(
            jnp.ones((8, LANES), jnp.float32),
            acc_ref[...],
            (((1,), (1,)), ((), ())),
            precision=lax.Precision.HIGHEST,
            preferred_element_type=jnp.float32,
        )

    vmem = pl.BlockSpec(memory_space=pltpu.VMEM)
    return pl.pallas_call(
        body,
        in_specs=[pl.BlockSpec(memory_space=pltpu.SMEM), vmem, vmem, vmem],
        out_specs=(vmem, vmem),
        out_shape=(
            jax.ShapeDtypeStruct((modes * per_mode, LANES), jnp.bfloat16),
            jax.ShapeDtypeStruct((8, LANES), jnp.float32),
        ),
        scratch_shapes=[
            pltpu.VMEM((modes * per_mode, LANES), jnp.float32),
            pltpu.VMEM((4 * modes, LANES), jnp.float32),
        ],
        name="transform",
    )(group, gathered, multipliers, weights)


def unpack(received, groups):
    _, outer, inner, lanes = received.shape
    per_step = 5

    def body(y_ref, o_ref):
        for s in range(groups):
            o_ref[:, s * inner : (s + 1) * inner, :] = y_ref[s].astype(jnp.float32)

    return pl.pallas_call(
        body,
        grid=(outer // per_step,),
        in_specs=[pl.BlockSpec((groups, per_step, inner, lanes), lambda k: (0, k, 0, 0))],
        out_specs=pl.BlockSpec((per_step, groups * inner, lanes), lambda k: (k, 0, 0)),
        out_shape=jax.ShapeDtypeStruct((outer, groups * inner, lanes), jnp.float32),
        name="unpack",
    )(received)


def on_device(snapshots, quad_weights, spectral_indices):
    point_count = snapshots.shape[2]
    groups = lax.axis_size("ta")
    me = lax.axis_index("ta")
    own = RETAINED_MODES // groups
    piece = point_count // groups
    tiles = piece // LANES
    temporal_locations = jnp.arange(RECORD_LENGTH, dtype=jnp.int32)
    multipliers = make_rotation_multipliers(spectral_indices, temporal_locations)

    packed = pack(jnp.transpose(snapshots, (1, 0, 2)), groups)
    gathered = lax.all_to_all(packed, "ta", split_axis=0, concat_axis=0, tiled=True)
    weights = quad_weights.reshape(point_count // LANES, LANES)
    payload, partial = transform(gathered, multipliers, weights, me[None].astype(jnp.int32))
    payload = payload.reshape(groups, own * SEGMENT_NUMBER * VARS, tiles * 2, LANES)
    received = lax.all_to_all(payload, "ta", split_axis=0, concat_axis=0, tiled=True)

    summed = lax.psum(partial, ("px", "py", "ta"))
    total_points = point_count * lax.axis_size("px") * lax.axis_size("py")
    terms = lax.dynamic_slice_in_dim(summed[0].reshape(4, RETAINED_MODES), me * own, own, axis=1)
    terms = terms / jnp.float32(total_points * VARS)
    p00, p11, real, imag = terms[0], terms[1], terms[2], terms[3]
    zero = jnp.zeros_like(p00)
    gram = jnp.stack([p00, zero, real, imag, real, -imag, p11, zero], axis=-1)
    gram = gram.reshape(own, SEGMENT_NUMBER, SEGMENT_NUMBER, 2)

    spectra = unpack(received, groups)
    spectra = spectra.reshape(own, SEGMENT_NUMBER, VARS, point_count // LANES, 2, LANES)
    spectra = jnp.transpose(spectra, (0, 1, 4, 2, 3, 5)).reshape(own, SEGMENT_NUMBER, 2, VARS, point_count)
    return (spectra, gram)


def solution(mesh):
    return jax.shard_map(
        on_device,
        mesh=mesh,
        in_specs=(P("ta", None, ("px", "py")), P(("px", "py")), P()),
        out_specs=(P("ta", None, None, None, ("px", "py")), P("ta", None, None, None)),
        check_vma=False,
    )
```

```python
import math

import jax
import jax.numpy as jnp
from jax import lax
from jax.experimental import pallas as pl
from jax.experimental.pallas import tpu as pltpu
from jax.sharding import PartitionSpec as P


VARS = 5
BLK = 256
HOP = 128
SEGMENT_NUMBER = 2
RECORD_LENGTH = 384
RETAINED_MODES = 32
LANES = 128
VMEM_LIMIT = 16 << 20
EXTRA = 8


def make_rotation_multipliers(spectral_indices, temporal_locations):
    segment_beginnings = jnp.arange(SEGMENT_NUMBER, dtype=jnp.int32) * HOP
    segment_shifts = temporal_locations[None, :] - segment_beginnings[:, None]
    inside = (segment_shifts >= 0) & (segment_shifts < BLK)
    window = 0.5 - 0.5 * jnp.cos(2.0 * math.pi * segment_shifts.astype(jnp.float32) / BLK)
    window = jnp.where(inside, window, jnp.float32(0.0)) / jnp.sqrt(jnp.float32(3.0 * BLK / 8.0))
    phases = jnp.mod(spectral_indices[None, :, None] * segment_shifts[:, None, :], BLK)
    angles = 2.0 * math.pi * phases.astype(jnp.float32) / BLK
    real_part = jnp.cos(angles) * window[:, None]
    imag_part = -jnp.sin(angles) * window[:, None]
    return (
        jnp.stack([real_part, imag_part], axis=0)
        .reshape(2 * SEGMENT_NUMBER * RETAINED_MODES, temporal_locations.shape[0])
        .astype(jnp.bfloat16)
    )


def pack(shard, groups):
    variables, times, points = shard.shape
    piece = points // groups

    def body(x_ref, o_ref, held, in_sem, out_sem):
        def take(d):
            return pltpu.make_async_copy(x_ref.at[:, :, pl.ds(d * piece, piece)], held.at[d], in_sem.at[d])

        def put(d):
            return pltpu.make_async_copy(held.at[d], o_ref.at[d], out_sem.at[d])

        for d in range(groups):
            take(d).start()
        for d in range(groups):
            take(d).wait()
            put(d).start()
        for d in range(groups):
            put(d).wait()

    shape = (groups, variables, times, piece)
    return pl.pallas_call(
        body,
        in_specs=[pl.BlockSpec(memory_space=pltpu.HBM)],
        out_specs=pl.BlockSpec(memory_space=pltpu.HBM),
        out_shape=jax.ShapeDtypeStruct(shape, shard.dtype),
        scratch_shapes=[
            pltpu.VMEM(shape, shard.dtype),
            pltpu.SemaphoreType.DMA((groups,)),
            pltpu.SemaphoreType.DMA((groups,)),
        ],
        name="pack",
    )(shard)


def transform(gathered, multipliers, weights, group):
    groups, variables, times, piece = gathered.shape
    tiles = piece // LANES
    modes = RETAINED_MODES
    own = modes // groups
    per_mode = SEGMENT_NUMBER * variables * tiles * 2
    height = own * per_mode + EXTRA

    def body(g_ref, x_ref, m_ref, w_ref, z_ref, f_ref, acc_ref):
        m = m_ref[...]
        acc_ref[...] = jnp.zeros_like(acc_ref)
        sw = jnp.sqrt(w_ref[pl.ds(g_ref[0] * tiles, tiles), :])
        for v in range(variables):
            x = x_ref[:, v].reshape(groups * times, piece)
            s = jnp.dot(m, x, preferred_element_type=jnp.float32)
            for j in range(tiles):
                q = s[:, j * LANES : (j + 1) * LANES] * sw[j : j + 1, :]
                parts = {}
                for c in range(2):
                    for b in range(SEGMENT_NUMBER):
                        at = (c * SEGMENT_NUMBER + b) * modes
                        part = q[at : at + modes]
                        parts[c, b] = part
                        for k in range(own):
                            first = k * per_mode + (b * variables + v) * tiles * 2 + j * 2 + c
                            f_ref[pl.ds(first, groups, stride=height), :] = part[k * groups : (k + 1) * groups]
                r0, r1, i0, i1 = parts[0, 0], parts[0, 1], parts[1, 0], parts[1, 1]
                acc_ref[0:modes] += r0 * r0 + i0 * i0
                acc_ref[modes : 2 * modes] += r1 * r1 + i1 * i1
                acc_ref[2 * modes : 3 * modes] += r0 * r1 + i0 * i1
                acc_ref[3 * modes : 4 * modes] += r0 * i1 - i0 * r1
        total = lax.dot_general(
            jnp.ones((EXTRA, LANES), jnp.float32),
            acc_ref[...],
            (((1,), (1,)), ((), ())),
            precision=lax.Precision.HIGHEST,
            preferred_element_type=jnp.float32,
        )
        rounded = total.astype(jnp.bfloat16).astype(jnp.float32)
        row = lax.broadcasted_iota(jnp.int32, total.shape, 0)
        tail = jnp.where(row == 0, rounded, jnp.where(row == 1, total - rounded, 0.0))
        for d in range(groups):
            f_ref[d * height + own * per_mode : (d + 1) * height, :] = tail
        z_ref[...] = f_ref[...].astype(z_ref.dtype)

    vmem = pl.BlockSpec(memory_space=pltpu.VMEM)
    return pl.pallas_call(
        body,
        in_specs=[pl.BlockSpec(memory_space=pltpu.SMEM), vmem, vmem, vmem],
        out_specs=vmem,
        out_shape=jax.ShapeDtypeStruct((groups * height, LANES), jnp.bfloat16),
        scratch_shapes=[
            pltpu.VMEM((groups * height, LANES), jnp.float32),
            pltpu.VMEM((4 * modes, LANES), jnp.float32),
        ],
        compiler_params=pltpu.CompilerParams(vmem_limit_bytes=VMEM_LIMIT),
        name="transform",
    )(group, gathered, multipliers, weights).reshape(groups, height, LANES)


def unpack(received, rows, inner):
    groups, _, lanes = received.shape
    outer = rows // inner
    per_step = 5

    def body(y_ref, o_ref):
        for s in range(groups):
            o_ref[:, s * inner : (s + 1) * inner, :] = y_ref[s].astype(jnp.float32).reshape(per_step, inner, lanes)

    return pl.pallas_call(
        body,
        grid=(outer // per_step,),
        in_specs=[pl.BlockSpec((groups, per_step * inner, lanes), lambda k: (0, k, 0))],
        out_specs=pl.BlockSpec((per_step, groups * inner, lanes), lambda k: (k, 0, 0)),
        out_shape=jax.ShapeDtypeStruct((outer, groups * inner, lanes), jnp.float32),
        compiler_params=pltpu.CompilerParams(vmem_limit_bytes=VMEM_LIMIT),
        name="unpack",
    )(received)


def gram_choice(me, own, terms):
    shape = (own, SEGMENT_NUMBER, SEGMENT_NUMBER, 2, LANES)
    f, b, b2, part, lane = (lax.broadcasted_iota(jnp.int32, shape, d) for d in range(5))
    q = jnp.where(b == b2, b, 2 + part)
    sign = jnp.where(part == 0, 1.0, (b2 - b).astype(jnp.float32))
    return jnp.where(lane == q * RETAINED_MODES + f * (RETAINED_MODES // own) + me, sign / jnp.float32(terms), 0.0)


def on_device(snapshots, quad_weights, spectral_indices):
    point_count = snapshots.shape[2]
    groups = lax.axis_size("ta")
    me = lax.axis_index("ta")
    own = RETAINED_MODES // groups
    piece = point_count // groups
    tiles = piece // LANES
    split = ("px", "py")
    copies = lax.axis_size(split)
    temporal_locations = jnp.arange(RECORD_LENGTH, dtype=jnp.int32)
    by_place = spectral_indices.reshape(groups, own).T.reshape(RETAINED_MODES)
    multipliers = make_rotation_multipliers(by_place, temporal_locations)

    packed = pack(jnp.transpose(snapshots, (1, 0, 2)), groups)
    gathered = lax.all_to_all(packed, "ta", split_axis=0, concat_axis=0, tiled=True)
    weights = quad_weights.reshape(point_count // LANES, LANES)
    payload = transform(gathered, multipliers, weights, me[None].astype(jnp.int32))
    received = lax.all_to_all(payload, "ta", split_axis=0, concat_axis=0, tiled=True)

    rows = own * SEGMENT_NUMBER * VARS * tiles * 2
    partial = jnp.sum(received[:, rows : rows + 2].astype(jnp.float32), axis=(0, 1))
    partial = jnp.broadcast_to(partial[None, None], (copies, 1, LANES))
    partial = lax.all_to_all(partial, split, split_axis=0, concat_axis=0, tiled=True)
    choice = gram_choice(me, own, point_count * copies * VARS)
    gram = jnp.sum(choice * jnp.sum(partial, axis=(0, 1)), axis=-1)

    spectra = unpack(received, rows, tiles * 2)
    spectra = spectra.reshape(own, SEGMENT_NUMBER, VARS, point_count // LANES, 2, LANES)
    spectra = jnp.transpose(spectra, (0, 1, 4, 2, 3, 5)).reshape(own, SEGMENT_NUMBER, 2, VARS, point_count)
    return (spectra, gram)


def solution(mesh):
    return jax.shard_map(
        on_device,
        mesh=mesh,
        in_specs=(P("ta", None, ("px", "py")), P(("px", "py")), P()),
        out_specs=(P("ta", None, None, None, ("px", "py")), P("ta", None, None, None)),
        check_vma=False,
    )
```

```python
import math

import jax
import jax.numpy as jnp
import numpy as np
from jax import lax
from jax.experimental import pallas as pl
from jax.experimental.pallas import tpu as pltpu
from jax.sharding import PartitionSpec as P


VARS = 5
BLK = 256
HOP = 128
SEGMENT_NUMBER = 2
RECORD_LENGTH = 384
RETAINED_MODES = 32
LANES = 128
VMEM_LIMIT = 16 << 20
EXTRA = 8


def multipliers_of(index_ref, own):
    modes = index_ref.shape[0]
    places = modes // own
    row = lax.broadcasted_iota(jnp.int32, (modes, BLK), 0)
    lag = lax.broadcasted_iota(jnp.int32, (modes, BLK), 1)
    index = jnp.zeros((modes, BLK), jnp.int32)
    for f in range(modes):
        index = jnp.where(row == f % own * places + f // own, index_ref[f], index)
    window = 0.5 - 0.5 * jnp.cos(2.0 * math.pi * lag.astype(jnp.float32) / BLK)
    window = window / jnp.sqrt(jnp.float32(3.0 * BLK / 8.0))
    angles = 2.0 * math.pi * ((index * lag) & (BLK - 1)).astype(jnp.float32) / BLK
    return jnp.cos(angles) * window, -jnp.sin(angles) * window


def pack(shard, indices, weights, me, groups):
    variables, times, points = shard.shape
    piece = points // groups
    modes = indices.shape[0]

    tiles = piece // LANES

    def body(me_ref, index_hbm, w_hbm, x_hbm, o_ref, m_ref, r_ref, index_ref, w_ref, sem, index_sem, w_sem):
        get_index = pltpu.make_async_copy(index_hbm, index_ref, index_sem)
        get_weights = pltpu.make_async_copy(w_hbm, w_ref, w_sem)
        get_index.start()
        copies = [
            pltpu.make_async_copy(x_hbm.at[:, :, pl.ds(d * piece, piece)], o_ref.at[d], sem.at[d])
            for d in range(groups)
        ]
        for copy in copies:
            copy.start()
        get_weights.start()
        m_ref[...] = jnp.zeros_like(m_ref)
        get_index.wait()
        for c, part in enumerate(multipliers_of(index_ref, modes // groups)):
            for b in range(SEGMENT_NUMBER):
                at = (c * SEGMENT_NUMBER + b) * modes
                m_ref[at : at + modes, b * HOP : b * HOP + BLK] = part.astype(m_ref.dtype)
        get_weights.wait()
        r_ref[...] = jnp.sqrt(w_ref[pl.ds(me_ref[0] * tiles, tiles), :])
        for copy in copies:
            copy.wait()

    vmem = pl.BlockSpec(memory_space=pltpu.VMEM)
    smem = pl.BlockSpec(memory_space=pltpu.SMEM)
    hbm = pl.BlockSpec(memory_space=pltpu.HBM)
    arrays = [pltpu.with_memory_space_constraint(array, pltpu.HBM) for array in (indices, weights, shard)]
    return pl.pallas_call(
        body,
        in_specs=[smem, hbm, hbm, hbm],
        out_specs=(vmem, vmem, vmem),
        out_shape=(
            jax.ShapeDtypeStruct((groups, variables, times, piece), shard.dtype),
            jax.ShapeDtypeStruct((2 * SEGMENT_NUMBER * modes, RECORD_LENGTH), jnp.bfloat16),
            jax.ShapeDtypeStruct((tiles, LANES), jnp.float32),
        ),
        scratch_shapes=[
            pltpu.SMEM(indices.shape, indices.dtype),
            pltpu.VMEM(weights.shape, weights.dtype),
            pltpu.SemaphoreType.DMA((groups,)),
            pltpu.SemaphoreType.DMA,
            pltpu.SemaphoreType.DMA,
        ],
        compiler_params=pltpu.CompilerParams(vmem_limit_bytes=VMEM_LIMIT),
        name="pack",
    )(me, *arrays)


def transform(gathered, multipliers, roots):
    groups, variables, times, piece = gathered.shape
    tiles = piece // LANES
    modes = RETAINED_MODES
    own = modes // groups
    per_mode = SEGMENT_NUMBER * variables * tiles * 2
    height = own * per_mode + EXTRA

    def body(x_ref, m_ref, r_ref, z_ref, f_ref, acc_ref):
        m = m_ref[...]
        acc_ref[...] = jnp.zeros_like(acc_ref)
        for v in range(variables):
            x = x_ref[:, v].reshape(groups * times, piece)
            s = jnp.dot(m, x, preferred_element_type=jnp.float32)
            for j in range(tiles):
                q = s[:, j * LANES : (j + 1) * LANES] * r_ref[j : j + 1, :]
                parts = {}
                for c in range(2):
                    for b in range(SEGMENT_NUMBER):
                        at = (c * SEGMENT_NUMBER + b) * modes
                        part = q[at : at + modes]
                        parts[c, b] = part
                        for k in range(own):
                            first = k * per_mode + (b * variables + v) * tiles * 2 + j * 2 + c
                            f_ref[pl.ds(first, groups, stride=height), :] = part[k * groups : (k + 1) * groups]
                r0, r1, i0, i1 = parts[0, 0], parts[0, 1], parts[1, 0], parts[1, 1]
                acc_ref[0:modes] += r0 * r0 + i0 * i0
                acc_ref[modes : 2 * modes] += r1 * r1 + i1 * i1
                acc_ref[2 * modes : 3 * modes] += r0 * r1 + i0 * i1
                acc_ref[3 * modes : 4 * modes] += r0 * i1 - i0 * r1
        total = lax.dot_general(
            jnp.ones((EXTRA, LANES), jnp.float32),
            acc_ref[...],
            (((1,), (1,)), ((), ())),
            precision=lax.Precision.HIGHEST,
            preferred_element_type=jnp.float32,
        )
        rounded = total.astype(jnp.bfloat16).astype(jnp.float32)
        row = lax.broadcasted_iota(jnp.int32, total.shape, 0)
        tail = jnp.where(row == 0, rounded, jnp.where(row == 1, total - rounded, 0.0))
        for d in range(groups):
            f_ref[d * height + own * per_mode : (d + 1) * height, :] = tail
        z_ref[...] = f_ref[...].reshape(z_ref.shape).astype(z_ref.dtype)

    vmem = pl.BlockSpec(memory_space=pltpu.VMEM)
    return pl.pallas_call(
        body,
        in_specs=[vmem, vmem, vmem],
        out_specs=vmem,
        out_shape=jax.ShapeDtypeStruct((groups, height, LANES), jnp.bfloat16),
        scratch_shapes=[
            pltpu.VMEM((groups * height, LANES), jnp.float32),
            pltpu.VMEM((4 * modes, LANES), jnp.float32),
        ],
        compiler_params=pltpu.CompilerParams(vmem_limit_bytes=VMEM_LIMIT),
        name="transform",
    )(gathered, multipliers, roots)


def unpack(received, rows, inner):
    groups, _, lanes = received.shape
    outer = rows // inner
    per_step = 5

    def body(y_ref, o_ref):
        for s in range(groups):
            o_ref[:, s * inner : (s + 1) * inner, :] = y_ref[s].astype(jnp.float32).reshape(per_step, inner, lanes)

    return pl.pallas_call(
        body,
        grid=(outer // per_step,),
        in_specs=[pl.BlockSpec((groups, per_step * inner, lanes), lambda k: (0, k, 0))],
        out_specs=pl.BlockSpec((per_step, groups * inner, lanes), lambda k: (k, 0, 0)),
        out_shape=jax.ShapeDtypeStruct((outer, groups * inner, lanes), jnp.float32),
        compiler_params=pltpu.CompilerParams(vmem_limit_bytes=VMEM_LIMIT),
        name="unpack",
    )(received)


def sum_over(value, axis):
    size = lax.axis_size(axis)
    halvings = (1, 2, 6) if size == 8 else tuple(1 << k for k in range(size.bit_length() - 1))
    for apart in halvings:
        value = value + lax.ppermute(value, axis, [(d, d ^ apart) for d in range(size)])
    return value


def gram_of(sums, me, own, terms):
    shape = (own, SEGMENT_NUMBER, SEGMENT_NUMBER, 2, 1)
    f, b, b2, part, _ = np.indices(shape)
    first = (np.where(b == b2, b, 2 + part) * own + f) * (RETAINED_MODES // own)
    factor = np.where(part == 0, 1.0, b2 - b) / terms
    lane = lax.broadcasted_iota(jnp.int32, shape[:4] + (LANES,), 4)
    chosen = jnp.where(lane == jnp.asarray(first, jnp.int32) + me, sums, 0.0)
    return jnp.sum(chosen * jnp.asarray(factor, jnp.float32), axis=-1)


def on_device(snapshots, quad_weights, spectral_indices):
    point_count = snapshots.shape[2]
    groups = lax.axis_size("ta")
    me = lax.axis_index("ta").astype(jnp.int32)
    own = RETAINED_MODES // groups
    tiles = point_count // groups // LANES
    rows = own * SEGMENT_NUMBER * VARS * tiles * 2

    weights = quad_weights.reshape(point_count // LANES, LANES)
    packed, multipliers, roots = pack(jnp.transpose(snapshots, (1, 0, 2)), spectral_indices, weights, me[None], groups)
    gathered = lax.all_to_all(packed, "ta", split_axis=0, concat_axis=0, tiled=True)
    payload = transform(gathered, multipliers, roots)
    received = lax.all_to_all(payload, "ta", split_axis=0, concat_axis=0, tiled=True)

    sums = jnp.sum(received[:, rows : rows + 2].astype(jnp.float32), axis=0)
    sums = jnp.sum(sums, axis=0, keepdims=True)
    for axis in ("px", "py"):
        sums = sum_over(sums, axis)
    terms = point_count * lax.axis_size("px") * lax.axis_size("py") * VARS
    gram = gram_of(sums, me, own, terms)

    spectra = unpack(received, rows, tiles * 2)
    spectra = spectra.reshape(own, SEGMENT_NUMBER, VARS, point_count // LANES, 2, LANES)
    spectra = jnp.transpose(spectra, (0, 1, 4, 2, 3, 5)).reshape(own, SEGMENT_NUMBER, 2, VARS, point_count)
    return (spectra, gram)


def solution(mesh):
    return jax.shard_map(
        on_device,
        mesh=mesh,
        in_specs=(P("ta", None, ("px", "py")), P(("px", "py")), P()),
        out_specs=(P("ta", None, None, None, ("px", "py")), P("ta", None, None, None)),
        check_vma=False,
    )
```

```python
import math

import jax
import jax.numpy as jnp
import numpy as np
from jax import lax
from jax.experimental import pallas as pl
from jax.experimental.pallas import tpu as pltpu
from jax.sharding import PartitionSpec as P


VARS = 5
BLK = 256
HOP = 128
SEGMENT_NUMBER = 2
RECORD_LENGTH = 384
RETAINED_MODES = 32
LANES = 128
VMEM_LIMIT = 16 << 20
EXTRA = 8
SPREAD = (9, 7, 13, 11, 10, 5, 2, 0, 15, 14, 4, 3, 6, 12, 1, 8)
COLLECT = (9, 7, 13, 11, 10, 5, 2, 0, 15, 14, 4, 3, 6, 12, 1, 8)
POINTS = (12, 0, 1, 2, 3, 4, 5, 6, 7, 8, 9, 10, 11, 13, 14, 15)


def slots(order):
    return [order.index(d) for d in range(len(order))]


def slot_of(device, order):
    words = [sum(slot << 4 * k for k, slot in enumerate(slots(order)[at : at + 7])) for at in (0, 7, 14)]
    word = jnp.where(device < 7, words[0], jnp.where(device < 14, words[1], words[2]))
    return lax.shift_right_logical(word, 4 * lax.rem(device, 7)) & 15


def exchange(pieces, axes, order):
    groups = [list(order)] if len(order) == pieces.shape[0] else None
    return lax.all_to_all(pieces, axes, split_axis=0, concat_axis=0, tiled=True, axis_index_groups=groups)


def multipliers_of(index_ref, own):
    modes = index_ref.shape[0]
    places = modes // own
    row = lax.broadcasted_iota(jnp.int32, (modes, BLK), 0)
    lag = lax.broadcasted_iota(jnp.int32, (modes, BLK), 1)
    index = jnp.zeros((modes, BLK), jnp.int32)
    for f in range(modes):
        index = jnp.where(row == f % own * places + slots(COLLECT)[f // own], index_ref[f], index)
    window = 0.5 - 0.5 * jnp.cos(2.0 * math.pi * lag.astype(jnp.float32) / BLK)
    window = window / jnp.sqrt(jnp.float32(3.0 * BLK / 8.0))
    angles = 2.0 * math.pi * ((index * lag) & (BLK - 1)).astype(jnp.float32) / BLK
    return jnp.cos(angles) * window, -jnp.sin(angles) * window


def pack(shard, indices, weights, places, groups):
    variables, times, points = shard.shape
    piece = points // groups
    modes = indices.shape[0]

    tiles = piece // LANES

    def body(places_ref, index_hbm, w_hbm, x_hbm, o_ref, m_ref, r_ref, index_ref, w_ref, sem, index_sem, w_sem):
        get_index = pltpu.make_async_copy(index_hbm, index_ref, index_sem)
        get_weights = pltpu.make_async_copy(w_hbm, w_ref, w_sem)
        get_index.start()
        copies = [
            pltpu.make_async_copy(x_hbm.at[:, :, pl.ds(d * piece, piece)], o_ref.at[slots(SPREAD)[d]], sem.at[d])
            for d in range(groups)
        ]
        for copy in copies:
            copy.start()
        get_weights.start()
        m_ref[...] = jnp.zeros_like(m_ref)
        get_index.wait()
        for c, part in enumerate(multipliers_of(index_ref, modes // groups)):
            for b in range(SEGMENT_NUMBER):
                at = (c * SEGMENT_NUMBER + b) * modes
                m_ref[at : at + modes, b * HOP : b * HOP + BLK] = part.astype(m_ref.dtype)
        get_weights.wait()
        me = lax.div(places_ref[0], groups)
        r_ref[...] = jnp.sqrt(w_ref[pl.ds(me * tiles, tiles), :])
        for copy in copies:
            copy.wait()

    vmem = pl.BlockSpec(memory_space=pltpu.VMEM)
    smem = pl.BlockSpec(memory_space=pltpu.SMEM)
    hbm = pl.BlockSpec(memory_space=pltpu.HBM)
    arrays = [pltpu.with_memory_space_constraint(array, pltpu.HBM) for array in (indices, weights, shard)]
    return pl.pallas_call(
        body,
        in_specs=[smem, hbm, hbm, hbm],
        out_specs=(vmem, vmem, vmem),
        out_shape=(
            jax.ShapeDtypeStruct((groups, variables, times, piece), shard.dtype),
            jax.ShapeDtypeStruct((2 * SEGMENT_NUMBER * modes, RECORD_LENGTH), jnp.bfloat16),
            jax.ShapeDtypeStruct((tiles, LANES), jnp.float32),
        ),
        scratch_shapes=[
            pltpu.SMEM(indices.shape, indices.dtype),
            pltpu.VMEM(weights.shape, weights.dtype),
            pltpu.SemaphoreType.DMA((groups,)),
            pltpu.SemaphoreType.DMA,
            pltpu.SemaphoreType.DMA,
        ],
        compiler_params=pltpu.CompilerParams(vmem_limit_bytes=VMEM_LIMIT),
        name="pack",
    )(places, *arrays)


def transform(gathered, multipliers, roots):
    groups, variables, _, piece = gathered.shape
    tiles = piece // LANES
    modes = RETAINED_MODES
    own = modes // groups
    per_mode = SEGMENT_NUMBER * variables * tiles * 2
    height = own * per_mode + EXTRA

    def body(x_ref, m_ref, r_ref, z_ref, f_ref, acc_ref):
        m = m_ref[...]
        acc_ref[...] = jnp.zeros_like(acc_ref)
        for v in range(variables):
            x = jnp.concatenate([x_ref[slot, v] for slot in slots(SPREAD)], axis=0)
            s = jnp.dot(m, x, preferred_element_type=jnp.float32)
            for j in range(tiles):
                q = s[:, j * LANES : (j + 1) * LANES] * r_ref[j : j + 1, :]
                parts = {}
                for c in range(2):
                    for b in range(SEGMENT_NUMBER):
                        at = (c * SEGMENT_NUMBER + b) * modes
                        part = q[at : at + modes]
                        parts[c, b] = part
                        for k in range(own):
                            first = k * per_mode + (b * variables + v) * tiles * 2 + j * 2 + c
                            f_ref[pl.ds(first, groups, stride=height), :] = part[k * groups : (k + 1) * groups]
                r0, r1, i0, i1 = parts[0, 0], parts[0, 1], parts[1, 0], parts[1, 1]
                acc_ref[0:modes] += r0 * r0 + i0 * i0
                acc_ref[modes : 2 * modes] += r1 * r1 + i1 * i1
                acc_ref[2 * modes : 3 * modes] += r0 * r1 + i0 * i1
                acc_ref[3 * modes : 4 * modes] += r0 * i1 - i0 * r1
        total = lax.dot_general(
            jnp.ones((EXTRA, LANES), jnp.float32),
            acc_ref[...],
            (((1,), (1,)), ((), ())),
            precision=lax.Precision.HIGHEST,
            preferred_element_type=jnp.float32,
        )
        rounded = total.astype(jnp.bfloat16).astype(jnp.float32)
        row = lax.broadcasted_iota(jnp.int32, total.shape, 0)
        tail = jnp.where(row == 0, rounded, jnp.where(row == 1, total - rounded, 0.0))
        for d in range(groups):
            f_ref[d * height + own * per_mode : (d + 1) * height, :] = tail
        z_ref[...] = f_ref[...].reshape(z_ref.shape).astype(z_ref.dtype)

    vmem = pl.BlockSpec(memory_space=pltpu.VMEM)
    return pl.pallas_call(
        body,
        in_specs=[vmem, vmem, vmem],
        out_specs=vmem,
        out_shape=jax.ShapeDtypeStruct((groups, height, LANES), jnp.bfloat16),
        scratch_shapes=[
            pltpu.VMEM((groups * height, LANES), jnp.float32),
            pltpu.VMEM((4 * modes, LANES), jnp.float32),
        ],
        compiler_params=pltpu.CompilerParams(vmem_limit_bytes=VMEM_LIMIT),
        name="transform",
    )(gathered, multipliers, roots)


def unpack(received, rows, inner):
    groups, _, lanes = received.shape
    outer = rows // inner
    per_step = 5

    def body(y_ref, o_ref):
        for s in range(groups):
            o_ref[:, s * inner : (s + 1) * inner, :] = y_ref[slots(COLLECT)[s]].astype(jnp.float32).reshape(per_step, inner, lanes)

    return pl.pallas_call(
        body,
        grid=(outer // per_step,),
        in_specs=[pl.BlockSpec((groups, per_step * inner, lanes), lambda k: (0, k, 0))],
        out_specs=pl.BlockSpec((per_step, groups * inner, lanes), lambda k: (k, 0, 0)),
        out_shape=jax.ShapeDtypeStruct((outer, groups * inner, lanes), jnp.float32),
        compiler_params=pltpu.CompilerParams(vmem_limit_bytes=VMEM_LIMIT),
        name="unpack",
    )(received)


def gram_of(sums, slot, own, terms):
    shape = (own, SEGMENT_NUMBER, SEGMENT_NUMBER, 2, 1)
    f, b, b2, part, _ = np.indices(shape)
    first = (np.where(b == b2, b, 2 + part) * own + f) * (RETAINED_MODES // own)
    factor = np.where(part == 0, 1.0, b2 - b) / terms
    lane = lax.broadcasted_iota(jnp.int32, shape[:4] + (LANES,), 4)
    chosen = jnp.where(lane == jnp.asarray(first, jnp.int32) + slot, sums, 0.0)
    return jnp.sum(chosen * jnp.asarray(factor, jnp.float32), axis=-1)


def on_device(snapshots, quad_weights, spectral_indices):
    point_count = snapshots.shape[2]
    groups = lax.axis_size("ta")
    me = lax.axis_index("ta").astype(jnp.int32)
    own = RETAINED_MODES // groups
    tiles = point_count // groups // LANES
    rows = own * SEGMENT_NUMBER * VARS * tiles * 2

    weights = quad_weights.reshape(point_count // LANES, LANES)
    slot = slot_of(me, COLLECT)
    places = (me * groups + slot)[None]
    packed, multipliers, roots = pack(jnp.transpose(snapshots, (1, 0, 2)), spectral_indices, weights, places, groups)
    gathered = exchange(packed, "ta", SPREAD)
    payload = transform(gathered, multipliers, roots)
    received = exchange(payload, "ta", COLLECT)

    split = ("px", "py")
    copies = lax.axis_size(split)
    sums = jnp.sum(received[:, rows : rows + 2].astype(jnp.float32), axis=(0, 1))
    sums = jnp.broadcast_to(sums, (copies, 1, LANES))
    sums = jnp.sum(exchange(sums, split, POINTS), axis=0)
    terms = point_count * copies * VARS
    gram = gram_of(sums, slot, own, terms)

    spectra = unpack(received, rows, tiles * 2)
    spectra = spectra.reshape(own, SEGMENT_NUMBER, VARS, point_count // LANES, 2, LANES)
    spectra = jnp.transpose(spectra, (0, 1, 4, 2, 3, 5)).reshape(own, SEGMENT_NUMBER, 2, VARS, point_count)
    return (spectra, gram)


def solution(mesh):
    return jax.shard_map(
        on_device,
        mesh=mesh,
        in_specs=(P("ta", None, ("px", "py")), P(("px", "py")), P()),
        out_specs=(P("ta", None, None, None, ("px", "py")), P("ta", None, None, None)),
        check_vma=False,
    )
```

```python
import math

import jax
import jax.numpy as jnp
from jax import lax
from jax.experimental import pallas as pl
from jax.experimental.pallas import tpu as pltpu
from jax.sharding import PartitionSpec as P

VARS = 5
BLK = 256
HOP = 128
SEGMENT_NUMBER = 2
RECORD_LENGTH = 384
RETAINED_MODES = 32
LANES = 128
VMEM_LIMIT = 16 << 20
EXTRA = 8
SPREAD = (11, 10, 0, 15, 12, 14, 8, 4, 7, 5, 1, 2, 13, 3, 9, 6)
COLLECT = (14, 7, 8, 11, 10, 5, 2, 0, 15, 9, 4, 3, 6, 12, 1, 13)
POINTS = (12, 0, 1, 2, 3, 4, 5, 6, 7, 8, 9, 10, 11, 13, 14, 15)


def slots(order):
    return [order.index(d) for d in range(len(order))]


def slot_of(device, order):
    words = [sum(slot << 4 * k for k, slot in enumerate(slots(order)[at : at + 7])) for at in (0, 7, 14)]
    word = jnp.where(device < 7, words[0], jnp.where(device < 14, words[1], words[2]))
    return lax.shift_right_logical(word, 4 * lax.rem(device, 7)) & 15


def exchange(pieces, axes, order):
    groups = [list(order)] if len(order) == pieces.shape[0] else None
    return lax.all_to_all(pieces, axes, split_axis=0, concat_axis=0, tiled=True, axis_index_groups=groups)


def cos_sin(turns):
    quarter = ((turns + 32) >> 6) & 3
    x = (((turns + 32) & 63) - 32).astype(jnp.float32) * jnp.float32(2.0 * math.pi / BLK)
    y = x * x
    cos = 1.0 + y * (-1 / 2 + y * (1 / 24 + y * (-1 / 720 + y * (1 / 40320 - y * (1 / 3628800)))))
    sin = x * (1.0 + y * (-1 / 6 + y * (1 / 120 + y * (-1 / 5040 + y * (1 / 362880)))))
    odd = (quarter & 1) == 1
    cos, sin = jnp.where(odd, sin, cos), jnp.where(odd, cos, sin)
    return jnp.where((quarter == 1) | (quarter == 2), -cos, cos), jnp.where(quarter >= 2, -sin, sin)


def multipliers_of(index_ref, own):
    modes = index_ref.shape[0]
    places = modes // own
    row = lax.broadcasted_iota(jnp.int32, (modes, BLK), 0)
    lag = lax.broadcasted_iota(jnp.int32, (modes, BLK), 1)
    index = jnp.zeros((modes, BLK), jnp.int32)
    for f in range(modes):
        index = jnp.where(row == f % own * places + slots(COLLECT)[f // own], index_ref[f], index)
    window = 0.5 - 0.5 * cos_sin(lax.broadcasted_iota(jnp.int32, (8, BLK), 1))[0]
    window = (window / jnp.sqrt(jnp.float32(3.0 * BLK / 8.0)))[:1]
    cos, sin = cos_sin((index * lag) & (BLK - 1))
    return cos * window, -sin * window


def pack(shard, indices, weights, places, groups):
    variables, times, points = shard.shape
    piece = points // groups
    modes = indices.shape[0]

    tiles = piece // LANES

    def body(places_ref, index_hbm, w_hbm, x_hbm, o_ref, m_ref, r_ref, index_ref, w_ref, sem, index_sem, w_sem):
        get_index = pltpu.make_async_copy(index_hbm, index_ref, index_sem)
        get_weights = pltpu.make_async_copy(w_hbm, w_ref, w_sem)
        get_index.start()
        copies = [
            pltpu.make_async_copy(x_hbm.at[:, :, pl.ds(d * piece, piece)], o_ref.at[slots(SPREAD)[d]], sem.at[d])
            for d in range(groups)
        ]
        for copy in copies:
            copy.start()
        get_weights.start()
        m_ref[...] = jnp.zeros_like(m_ref)
        get_index.wait()
        for c, part in enumerate(multipliers_of(index_ref, modes // groups)):
            for b in range(SEGMENT_NUMBER):
                at = (c * SEGMENT_NUMBER + b) * modes
                m_ref[at : at + modes, b * HOP : b * HOP + BLK] = part.astype(m_ref.dtype)
        get_weights.wait()
        me = lax.div(places_ref[0], groups)
        r_ref[...] = jnp.sqrt(w_ref[pl.ds(me * tiles, tiles), :])
        for copy in copies:
            copy.wait()

    vmem = pl.BlockSpec(memory_space=pltpu.VMEM)
    smem = pl.BlockSpec(memory_space=pltpu.SMEM)
    hbm = pl.BlockSpec(memory_space=pltpu.HBM)
    arrays = [pltpu.with_memory_space_constraint(array, pltpu.HBM) for array in (indices, weights, shard)]
    return pl.pallas_call(
        body,
        in_specs=[smem, hbm, hbm, hbm],
        out_specs=(vmem, vmem, vmem),
        out_shape=(
            jax.ShapeDtypeStruct((groups, variables, times, piece), shard.dtype),
            jax.ShapeDtypeStruct((2 * SEGMENT_NUMBER * modes, RECORD_LENGTH), jnp.bfloat16),
            jax.ShapeDtypeStruct((tiles, LANES), jnp.float32),
        ),
        scratch_shapes=[
            pltpu.SMEM(indices.shape, indices.dtype),
            pltpu.VMEM(weights.shape, weights.dtype),
            pltpu.SemaphoreType.DMA((groups,)),
            pltpu.SemaphoreType.DMA,
            pltpu.SemaphoreType.DMA,
        ],
        compiler_params=pltpu.CompilerParams(vmem_limit_bytes=VMEM_LIMIT),
        name="pack",
    )(places, *arrays)


def transform(gathered, multipliers, roots):
    groups, variables, times, piece = gathered.shape
    tiles = piece // LANES
    modes = RETAINED_MODES
    own = modes // groups
    per_mode = SEGMENT_NUMBER * variables * tiles * 2
    height = own * per_mode + EXTRA

    def body(x_ref, m_ref, r_ref, z_ref, f_ref, acc_ref):
        m = m_ref[...]
        acc_ref[...] = jnp.zeros_like(acc_ref)
        for v in range(variables):
            x = jnp.concatenate([x_ref[slot, v] for slot in slots(SPREAD)], axis=0)
            s = jnp.dot(m, x, preferred_element_type=jnp.float32)
            for j in range(tiles):
                q = s[:, j * LANES : (j + 1) * LANES] * r_ref[j : j + 1, :]
                parts = {}
                for c in range(2):
                    for b in range(SEGMENT_NUMBER):
                        at = (c * SEGMENT_NUMBER + b) * modes
                        part = q[at : at + modes]
                        parts[c, b] = part
                        for k in range(own):
                            first = k * per_mode + (b * variables + v) * tiles * 2 + j * 2 + c
                            f_ref[pl.ds(first, groups, stride=height), :] = part[k * groups : (k + 1) * groups]
                r0, r1, i0, i1 = parts[0, 0], parts[0, 1], parts[1, 0], parts[1, 1]
                acc_ref[0:modes] += r0 * r0 + i0 * i0
                acc_ref[modes : 2 * modes] += r1 * r1 + i1 * i1
                acc_ref[2 * modes : 3 * modes] += r0 * r1 + i0 * i1
                acc_ref[3 * modes : 4 * modes] += r0 * i1 - i0 * r1
        total = lax.dot_general(
            jnp.ones((EXTRA, LANES), jnp.float32),
            acc_ref[...],
            (((1,), (1,)), ((), ())),
            precision=lax.Precision.HIGHEST,
            preferred_element_type=jnp.float32,
        )
        rounded = total.astype(jnp.bfloat16).astype(jnp.float32)
        row = lax.broadcasted_iota(jnp.int32, total.shape, 0)
        tail = jnp.where(row == 0, rounded, jnp.where(row == 1, total - rounded, 0.0))
        for d in range(groups):
            f_ref[d * height + own * per_mode : (d + 1) * height, :] = tail
        z_ref[...] = f_ref[...].reshape(z_ref.shape).astype(z_ref.dtype)

    vmem = pl.BlockSpec(memory_space=pltpu.VMEM)
    return pl.pallas_call(
        body,
        in_specs=[vmem, vmem, vmem],
        out_specs=vmem,
        out_shape=jax.ShapeDtypeStruct((groups, height, LANES), jnp.bfloat16),
        scratch_shapes=[
            pltpu.VMEM((groups * height, LANES), jnp.float32),
            pltpu.VMEM((4 * modes, LANES), jnp.float32),
        ],
        compiler_params=pltpu.CompilerParams(vmem_limit_bytes=VMEM_LIMIT),
        name="transform",
    )(gathered, multipliers, roots)


def unpack(received, rows, inner, copies):
    groups, _, lanes = received.shape
    outer = rows // inner

    def body(y_ref, o_ref, sums_ref):
        total = jnp.zeros((EXTRA, lanes), jnp.float32)
        for s, place in enumerate(slots(COLLECT)):
            piece = y_ref[place].astype(jnp.float32)
            o_ref[:, s * inner : (s + 1) * inner, :] = piece[:rows].reshape(outer, inner, lanes)
            total = total + piece[rows:]
        sums_ref[...] = jnp.broadcast_to((total[:1] + total[1:2])[None], sums_ref.shape)

    vmem = pl.BlockSpec(memory_space=pltpu.VMEM)
    return pl.pallas_call(
        body,
        in_specs=[vmem],
        out_specs=(vmem, vmem),
        out_shape=(
            pltpu.VMEM((outer, groups * inner, lanes), jnp.float32),
            pltpu.VMEM((copies, 1, lanes), jnp.float32),
        ),
        compiler_params=pltpu.CompilerParams(vmem_limit_bytes=VMEM_LIMIT),
        name="unpack",
    )(received)


def finish(spectra, sums, slot, groups, terms):
    own = RETAINED_MODES // groups
    entries = own * SEGMENT_NUMBER * SEGMENT_NUMBER
    lanes = sums.shape[-1]
    chunks = 4
    size = spectra.shape[0] // chunks

    def body(slot_ref, sums_ref, s_ref, o_hbm, gram_ref, sem):
        copies = []
        for k in range(chunks):
            part = pl.ds(k * size, size)
            copies.append(pltpu.make_async_copy(s_ref.at[part], o_hbm.at[part], sem.at[k]))
            copies[-1].start()
        total = sums_ref[0]
        for k in range(1, sums_ref.shape[0]):
            total = total + sums_ref[k]
        row = lax.broadcasted_iota(jnp.int32, (entries, lanes), 0)
        lane = lax.broadcasted_iota(jnp.int32, (entries, lanes), 1)
        f, b, b2 = row >> 2, (row >> 1) & 1, row & 1

        def chosen(q):
            there = lane == (q * own + f) * groups + slot_ref[0]
            return jnp.sum(jnp.where(there, total, 0.0), axis=1, keepdims=True) * jnp.float32(1.0 / terms)

        real = chosen(jnp.where(b == b2, b, 2))
        imag = chosen(3) * (b2 - b).astype(jnp.float32)
        both = jnp.where(lane == 0, real, imag)
        for k in range(entries // 2):
            gram_ref[k] = both[2 * k : 2 * k + 2, :2]
        for copy in copies:
            copy.wait()

    vmem = pl.BlockSpec(memory_space=pltpu.VMEM)
    return pl.pallas_call(
        body,
        in_specs=[pl.BlockSpec(memory_space=pltpu.SMEM), vmem, vmem],
        out_specs=(pl.BlockSpec(memory_space=pltpu.HBM), vmem),
        out_shape=(
            jax.ShapeDtypeStruct(spectra.shape, spectra.dtype),
            jax.ShapeDtypeStruct((entries // 2, 2, 2), jnp.float32),
        ),
        scratch_shapes=[pltpu.SemaphoreType.DMA((chunks,))],
        compiler_params=pltpu.CompilerParams(vmem_limit_bytes=VMEM_LIMIT),
        name="finish",
    )(slot, sums, spectra)


def on_device(snapshots, quad_weights, spectral_indices):
    point_count = snapshots.shape[2]
    groups = lax.axis_size("ta")
    me = lax.axis_index("ta").astype(jnp.int32)
    own = RETAINED_MODES // groups
    tiles = point_count // groups // LANES
    rows = own * SEGMENT_NUMBER * VARS * tiles * 2

    weights = quad_weights.reshape(point_count // LANES, LANES)
    slot = slot_of(me, COLLECT)
    places = (me * groups + slot)[None]
    packed, multipliers, roots = pack(jnp.transpose(snapshots, (1, 0, 2)), spectral_indices, weights, places, groups)
    with jax.named_scope("spread"):
        gathered = exchange(packed, "ta", SPREAD)
    payload = transform(gathered, multipliers, roots)
    with jax.named_scope("collect"):
        received = exchange(payload, "ta", COLLECT)

    split = ("px", "py")
    copies = lax.axis_size(split)
    spectra, sums = unpack(received, rows, tiles * 2, copies)
    with jax.named_scope("points"):
        sums = exchange(sums, split, POINTS)
    spectra, gram = finish(spectra, sums, slot[None], groups, point_count * copies * VARS)
    gram = gram.reshape(own, SEGMENT_NUMBER, SEGMENT_NUMBER, 2)
    spectra = spectra.reshape(own, SEGMENT_NUMBER, VARS, point_count // LANES, 2, LANES)
    spectra = jnp.transpose(spectra, (0, 1, 4, 2, 3, 5)).reshape(own, SEGMENT_NUMBER, 2, VARS, point_count)
    return (spectra, gram)


def solution(mesh):
    return jax.shard_map(
        on_device,
        mesh=mesh,
        in_specs=(P("ta", None, ("px", "py")), P(("px", "py")), P()),
        out_specs=(P("ta", None, None, None, ("px", "py")), P("ta", None, None, None)),
        check_vma=False,
    )
```

```python
import math

import jax
import jax.numpy as jnp
from jax import lax
from jax.experimental import pallas as pl
from jax.experimental.pallas import tpu as pltpu
from jax.sharding import PartitionSpec as P

VARS = 5
BLK = 256
HOP = 128
SEGMENT_NUMBER = 2
RECORD_LENGTH = 384
RETAINED_MODES = 32
LANES = 128
VMEM_LIMIT = 16 << 20
EXTRA = 8
SPREAD = (11, 10, 4, 15, 12, 14, 8, 0, 7, 5, 1, 2, 13, 3, 9, 6)
COLLECT = (14, 7, 2, 11, 10, 13, 3, 15, 1, 9, 5, 0, 6, 12, 8, 4)
POINTS = (12, 0, 1, 2, 3, 4, 5, 6, 7, 8, 9, 10, 11, 13, 14, 15)


def slots(order):
    return [order.index(d) for d in range(len(order))]


def slot_of(device, order):
    words = [sum(slot << 4 * k for k, slot in enumerate(slots(order)[at : at + 7])) for at in (0, 7, 14)]
    word = jnp.where(device < 7, words[0], jnp.where(device < 14, words[1], words[2]))
    return lax.shift_right_logical(word, 4 * lax.rem(device, 7)) & 15


def exchange(pieces, axes, order):
    groups = [list(order)] if len(order) == pieces.shape[0] else None
    return lax.all_to_all(pieces, axes, split_axis=0, concat_axis=0, tiled=True, axis_index_groups=groups)


def cos_sin(turns):
    quarter = ((turns + 32) >> 6) & 3
    x = (((turns + 32) & 63) - 32).astype(jnp.float32) * jnp.float32(2.0 * math.pi / BLK)
    y = x * x
    cos = 1.0 + y * (-1 / 2 + y * (1 / 24 + y * (-1 / 720 + y * (1 / 40320 - y * (1 / 3628800)))))
    sin = x * (1.0 + y * (-1 / 6 + y * (1 / 120 + y * (-1 / 5040 + y * (1 / 362880)))))
    odd = (quarter & 1) == 1
    cos, sin = jnp.where(odd, sin, cos), jnp.where(odd, cos, sin)
    return jnp.where((quarter == 1) | (quarter == 2), -cos, cos), jnp.where(quarter >= 2, -sin, sin)


def multipliers_of(index_ref, own):
    modes = index_ref.shape[0]
    places = modes // own
    row = lax.broadcasted_iota(jnp.int32, (modes, BLK), 0)
    lag = lax.broadcasted_iota(jnp.int32, (modes, BLK), 1)
    index = jnp.zeros((modes, BLK), jnp.int32)
    for f in range(modes):
        index = jnp.where(row == f % own * places + slots(COLLECT)[f // own], index_ref[f], index)
    window = 0.5 - 0.5 * cos_sin(lax.broadcasted_iota(jnp.int32, (8, BLK), 1))[0]
    window = (window / jnp.sqrt(jnp.float32(3.0 * BLK / 8.0)))[:1]
    cos, sin = cos_sin((index * lag) & (BLK - 1))
    return cos * window, -sin * window


def pack(shard, indices, weights, places, groups):
    variables, times, points = shard.shape
    piece = points // groups
    modes = indices.shape[0]

    tiles = piece // LANES

    def body(places_ref, index_hbm, w_hbm, x_hbm, o_ref, m_ref, r_ref, index_ref, w_ref, x_ref, sem, index_sem, w_sem):
        get_index = pltpu.make_async_copy(index_hbm, index_ref, index_sem)
        get_weights = pltpu.make_async_copy(w_hbm, w_ref, w_sem)
        get_index.start()
        copies = [pltpu.make_async_copy(x_hbm.at[v], x_ref.at[v], sem.at[v]) for v in range(variables)]
        for copy in copies:
            copy.start()
        get_weights.start()
        m_ref[...] = jnp.zeros_like(m_ref)
        get_index.wait()
        for c, part in enumerate(multipliers_of(index_ref, modes // groups)):
            for b in range(SEGMENT_NUMBER):
                at = (c * SEGMENT_NUMBER + b) * modes
                m_ref[at : at + modes, b * HOP : b * HOP + BLK] = part.astype(m_ref.dtype)
        get_weights.wait()
        me = lax.div(places_ref[0], groups)
        r_ref[...] = jnp.sqrt(w_ref[pl.ds(me * tiles, tiles), :])
        for v, copy in enumerate(copies):
            copy.wait()
            for d, slot in enumerate(slots(SPREAD)):
                o_ref[slot, v] = x_ref[v, :, d * piece : (d + 1) * piece]

    vmem = pl.BlockSpec(memory_space=pltpu.VMEM)
    smem = pl.BlockSpec(memory_space=pltpu.SMEM)
    hbm = pl.BlockSpec(memory_space=pltpu.HBM)
    arrays = [pltpu.with_memory_space_constraint(array, pltpu.HBM) for array in (indices, weights, shard)]
    return pl.pallas_call(
        body,
        in_specs=[smem, hbm, hbm, hbm],
        out_specs=(vmem, vmem, vmem),
        out_shape=(
            jax.ShapeDtypeStruct((groups, variables, times, piece), shard.dtype),
            jax.ShapeDtypeStruct((2 * SEGMENT_NUMBER * modes, RECORD_LENGTH), jnp.bfloat16),
            jax.ShapeDtypeStruct((tiles, LANES), jnp.float32),
        ),
        scratch_shapes=[
            pltpu.SMEM(indices.shape, indices.dtype),
            pltpu.VMEM(weights.shape, weights.dtype),
            pltpu.VMEM(shard.shape, shard.dtype),
            pltpu.SemaphoreType.DMA((variables,)),
            pltpu.SemaphoreType.DMA,
            pltpu.SemaphoreType.DMA,
        ],
        compiler_params=pltpu.CompilerParams(vmem_limit_bytes=VMEM_LIMIT),
        name="pack",
    )(places, *arrays)


def transform(gathered, multipliers, roots):
    groups, variables, times, piece = gathered.shape
    tiles = piece // LANES
    modes = RETAINED_MODES
    own = modes // groups
    per_mode = SEGMENT_NUMBER * variables * tiles * 2
    height = own * per_mode + EXTRA

    def body(x_ref, m_ref, r_ref, z_ref, f_ref, acc_ref):
        m = m_ref[...]
        acc_ref[...] = jnp.zeros_like(acc_ref)
        for v in range(variables):
            x = jnp.concatenate([x_ref[slot, v] for slot in slots(SPREAD)], axis=0)
            s = jnp.dot(m, x, preferred_element_type=jnp.float32)
            for j in range(tiles):
                q = s[:, j * LANES : (j + 1) * LANES] * r_ref[j : j + 1, :]
                parts = {}
                for c in range(2):
                    for b in range(SEGMENT_NUMBER):
                        at = (c * SEGMENT_NUMBER + b) * modes
                        part = q[at : at + modes]
                        parts[c, b] = part
                        for k in range(own):
                            first = k * per_mode + (b * variables + v) * tiles * 2 + j * 2 + c
                            f_ref[pl.ds(first, groups, stride=height), :] = part[k * groups : (k + 1) * groups]
                r0, r1, i0, i1 = parts[0, 0], parts[0, 1], parts[1, 0], parts[1, 1]
                acc_ref[0:modes] += r0 * r0 + i0 * i0
                acc_ref[modes : 2 * modes] += r1 * r1 + i1 * i1
                acc_ref[2 * modes : 3 * modes] += r0 * r1 + i0 * i1
                acc_ref[3 * modes : 4 * modes] += r0 * i1 - i0 * r1
        total = lax.dot_general(
            jnp.ones((EXTRA, LANES), jnp.float32),
            acc_ref[...],
            (((1,), (1,)), ((), ())),
            precision=lax.Precision.HIGHEST,
            preferred_element_type=jnp.float32,
        )
        rounded = total.astype(jnp.bfloat16).astype(jnp.float32)
        row = lax.broadcasted_iota(jnp.int32, total.shape, 0)
        tail = jnp.where(row == 0, rounded, jnp.where(row == 1, total - rounded, 0.0))
        for d in range(groups):
            f_ref[d * height + own * per_mode : (d + 1) * height, :] = tail
        z_ref[...] = f_ref[...].reshape(z_ref.shape).astype(z_ref.dtype)

    vmem = pl.BlockSpec(memory_space=pltpu.VMEM)
    return pl.pallas_call(
        body,
        in_specs=[vmem, vmem, vmem],
        out_specs=vmem,
        out_shape=jax.ShapeDtypeStruct((groups, height, LANES), jnp.bfloat16),
        scratch_shapes=[
            pltpu.VMEM((groups * height, LANES), jnp.float32),
            pltpu.VMEM((4 * modes, LANES), jnp.float32),
        ],
        compiler_params=pltpu.CompilerParams(vmem_limit_bytes=VMEM_LIMIT),
        name="transform",
    )(gathered, multipliers, roots)


def unpack(received, rows, inner, copies):
    groups, _, lanes = received.shape
    outer = rows // inner

    def body(y_ref, o_ref, sums_ref):
        total = jnp.zeros((EXTRA, lanes), jnp.float32)
        for s, place in enumerate(slots(COLLECT)):
            piece = y_ref[place].astype(jnp.float32)
            o_ref[:, s * inner : (s + 1) * inner, :] = piece[:rows].reshape(outer, inner, lanes)
            total = total + piece[rows:]
        sums_ref[...] = jnp.broadcast_to((total[:1] + total[1:2])[None], sums_ref.shape)

    vmem = pl.BlockSpec(memory_space=pltpu.VMEM)
    return pl.pallas_call(
        body,
        in_specs=[vmem],
        out_specs=(vmem, vmem),
        out_shape=(
            pltpu.VMEM((outer, groups * inner, lanes), jnp.float32),
            pltpu.VMEM((copies, 1, lanes), jnp.float32),
        ),
        compiler_params=pltpu.CompilerParams(vmem_limit_bytes=VMEM_LIMIT),
        name="unpack",
    )(received)


def finish(spectra, sums, slot, groups, terms):
    own = RETAINED_MODES // groups
    entries = own * SEGMENT_NUMBER * SEGMENT_NUMBER
    lanes = sums.shape[-1]
    chunks = 4
    size = spectra.shape[0] // chunks

    def body(slot_ref, sums_ref, s_ref, o_hbm, gram_ref, sem):
        copies = []
        for k in range(chunks):
            part = pl.ds(k * size, size)
            copies.append(pltpu.make_async_copy(s_ref.at[part], o_hbm.at[part], sem.at[k]))
            copies[-1].start()
        total = sums_ref[0]
        for k in range(1, sums_ref.shape[0]):
            total = total + sums_ref[k]
        row = lax.broadcasted_iota(jnp.int32, (entries, lanes), 0)
        lane = lax.broadcasted_iota(jnp.int32, (entries, lanes), 1)
        f, b, b2 = row >> 2, (row >> 1) & 1, row & 1

        def chosen(q):
            there = lane == (q * own + f) * groups + slot_ref[0]
            return jnp.sum(jnp.where(there, total, 0.0), axis=1, keepdims=True) * jnp.float32(1.0 / terms)

        real = chosen(jnp.where(b == b2, b, 2))
        imag = chosen(3) * (b2 - b).astype(jnp.float32)
        both = jnp.where(lane == 0, real, imag)
        for k in range(entries // 2):
            gram_ref[k] = both[2 * k : 2 * k + 2, :2]
        for copy in copies:
            copy.wait()

    vmem = pl.BlockSpec(memory_space=pltpu.VMEM)
    return pl.pallas_call(
        body,
        in_specs=[pl.BlockSpec(memory_space=pltpu.SMEM), vmem, vmem],
        out_specs=(pl.BlockSpec(memory_space=pltpu.HBM), vmem),
        out_shape=(
            jax.ShapeDtypeStruct(spectra.shape, spectra.dtype),
            jax.ShapeDtypeStruct((entries // 2, 2, 2), jnp.float32),
        ),
        scratch_shapes=[pltpu.SemaphoreType.DMA((chunks,))],
        compiler_params=pltpu.CompilerParams(vmem_limit_bytes=VMEM_LIMIT),
        name="finish",
    )(slot, sums, spectra)


def on_device(snapshots, quad_weights, spectral_indices):
    point_count = snapshots.shape[2]
    groups = lax.axis_size("ta")
    me = lax.axis_index("ta").astype(jnp.int32)
    own = RETAINED_MODES // groups
    tiles = point_count // groups // LANES
    rows = own * SEGMENT_NUMBER * VARS * tiles * 2

    weights = quad_weights.reshape(point_count // LANES, LANES)
    slot = slot_of(me, COLLECT)
    places = (me * groups + slot)[None]
    packed, multipliers, roots = pack(jnp.transpose(snapshots, (1, 0, 2)), spectral_indices, weights, places, groups)
    with jax.named_scope("spread"):
        gathered = exchange(packed, "ta", SPREAD)
    payload = transform(gathered, multipliers, roots)
    with jax.named_scope("collect"):
        received = exchange(payload, "ta", COLLECT)

    split = ("px", "py")
    copies = lax.axis_size(split)
    spectra, sums = unpack(received, rows, tiles * 2, copies)
    with jax.named_scope("points"):
        sums = exchange(sums, split, POINTS)
    spectra, gram = finish(spectra, sums, slot[None], groups, point_count * copies * VARS)
    gram = gram.reshape(own, SEGMENT_NUMBER, SEGMENT_NUMBER, 2)
    spectra = spectra.reshape(own, SEGMENT_NUMBER, VARS, point_count // LANES, 2, LANES)
    spectra = jnp.transpose(spectra, (0, 1, 4, 2, 3, 5)).reshape(own, SEGMENT_NUMBER, 2, VARS, point_count)
    return (spectra, gram)


def solution(mesh):
    return jax.shard_map(
        on_device,
        mesh=mesh,
        in_specs=(P("ta", None, ("px", "py")), P(("px", "py")), P()),
        out_specs=(P("ta", None, None, None, ("px", "py")), P("ta", None, None, None)),
        check_vma=False,
    )
```

```python
import math

import jax
import jax.numpy as jnp
from jax import lax
from jax.experimental import pallas as pl
from jax.experimental.pallas import tpu as pltpu
from jax.sharding import PartitionSpec as P

VARS = 5
BLK = 256
HOP = 128
SEGMENT_NUMBER = 2
RECORD_LENGTH = 384
RETAINED_MODES = 32
LANES = 128
VMEM_LIMIT = 16 << 20
EXTRA = 8
SPREAD = (11, 10, 4, 15, 12, 14, 8, 0, 7, 5, 1, 2, 13, 3, 9, 6)
COLLECT = (14, 7, 2, 11, 10, 13, 3, 15, 1, 9, 5, 0, 6, 12, 8, 4)
POINTS = (12, 0, 1, 2, 3, 4, 5, 6, 7, 8, 9, 10, 11, 13, 14, 15)


def slots(order):
    return [order.index(d) for d in range(len(order))]


def slot_of(device, order):
    words = [sum(slot << 4 * k for k, slot in enumerate(slots(order)[at : at + 7])) for at in (0, 7, 14)]
    word = jnp.where(device < 7, words[0], jnp.where(device < 14, words[1], words[2]))
    return lax.shift_right_logical(word, 4 * lax.rem(device, 7)) & 15


def exchange(pieces, axes, order):
    groups = [list(order)] if len(order) == pieces.shape[0] else None
    return lax.all_to_all(pieces, axes, split_axis=0, concat_axis=0, tiled=True, axis_index_groups=groups)


def cos_sin(turns):
    quarter = ((turns + 32) >> 6) & 3
    x = (((turns + 32) & 63) - 32).astype(jnp.float32) * jnp.float32(2.0 * math.pi / BLK)
    y = x * x
    cos = 1.0 + y * (-1 / 2 + y * (1 / 24 + y * (-1 / 720 + y * (1 / 40320 - y * (1 / 3628800)))))
    sin = x * (1.0 + y * (-1 / 6 + y * (1 / 120 + y * (-1 / 5040 + y * (1 / 362880)))))
    odd = (quarter & 1) == 1
    cos, sin = jnp.where(odd, sin, cos), jnp.where(odd, cos, sin)
    return jnp.where((quarter == 1) | (quarter == 2), -cos, cos), jnp.where(quarter >= 2, -sin, sin)


def multipliers_of(index_ref, own):
    modes = index_ref.shape[0]
    places = modes // own
    row = lax.broadcasted_iota(jnp.int32, (modes, BLK), 0)
    lag = lax.broadcasted_iota(jnp.int32, (modes, BLK), 1)
    index = jnp.zeros((modes, BLK), jnp.int32)
    for f in range(modes):
        index = jnp.where(row == f % own * places + slots(COLLECT)[f // own], index_ref[f], index)
    window = 0.5 - 0.5 * cos_sin(lax.broadcasted_iota(jnp.int32, (8, BLK), 1))[0]
    window = (window / jnp.sqrt(jnp.float32(3.0 * BLK / 8.0)))[:1]
    cos, sin = cos_sin((index * lag) & (BLK - 1))
    return cos * window, -sin * window


def pack(shard, indices, weights, places, groups):
    variables, times, points = shard.shape
    piece = points // groups
    modes = indices.shape[0]

    tiles = piece // LANES

    def body(places_ref, index_hbm, w_hbm, x_hbm, o_ref, m_ref, r_ref, index_ref, w_ref, x_ref, sem, index_sem, w_sem):
        get_index = pltpu.make_async_copy(index_hbm, index_ref, index_sem)
        get_weights = pltpu.make_async_copy(w_hbm, w_ref, w_sem)
        get_index.start()
        copies = [pltpu.make_async_copy(x_hbm.at[v], x_ref.at[v], sem.at[v]) for v in range(variables)]
        for copy in copies:
            copy.start()
        get_weights.start()
        m_ref[...] = jnp.zeros_like(m_ref)
        get_index.wait()
        for c, part in enumerate(multipliers_of(index_ref, modes // groups)):
            for b in range(SEGMENT_NUMBER):
                at = (c * SEGMENT_NUMBER + b) * modes
                m_ref[at : at + modes, b * HOP : b * HOP + BLK] = part.astype(m_ref.dtype)
        get_weights.wait()
        me = lax.div(places_ref[0], groups)
        r_ref[...] = jnp.sqrt(w_ref[pl.ds(me * tiles, tiles), :])
        for v, copy in enumerate(copies):
            copy.wait()
            for d, slot in enumerate(slots(SPREAD)):
                o_ref[slot, v] = x_ref[v, :, d * piece : (d + 1) * piece]

    vmem = pl.BlockSpec(memory_space=pltpu.VMEM)
    smem = pl.BlockSpec(memory_space=pltpu.SMEM)
    hbm = pl.BlockSpec(memory_space=pltpu.HBM)
    arrays = [pltpu.with_memory_space_constraint(array, pltpu.HBM) for array in (indices, weights, shard)]
    return pl.pallas_call(
        body,
        in_specs=[smem, hbm, hbm, hbm],
        out_specs=(vmem, vmem, vmem),
        out_shape=(
            jax.ShapeDtypeStruct((groups, variables, times, piece), shard.dtype),
            jax.ShapeDtypeStruct((2 * SEGMENT_NUMBER * modes, RECORD_LENGTH), jnp.bfloat16),
            jax.ShapeDtypeStruct((tiles, LANES), jnp.float32),
        ),
        scratch_shapes=[
            pltpu.SMEM(indices.shape, indices.dtype),
            pltpu.VMEM(weights.shape, weights.dtype),
            pltpu.VMEM(shard.shape, shard.dtype),
            pltpu.SemaphoreType.DMA((variables,)),
            pltpu.SemaphoreType.DMA,
            pltpu.SemaphoreType.DMA,
        ],
        compiler_params=pltpu.CompilerParams(vmem_limit_bytes=VMEM_LIMIT),
        name="pack",
    )(places, *arrays)


def transform(gathered, multipliers, roots):
    groups, variables, times, piece = gathered.shape
    tiles = piece // LANES
    modes = RETAINED_MODES
    own = modes // groups
    per_mode = SEGMENT_NUMBER * variables * tiles * 2
    height = own * per_mode + EXTRA

    def body(x_ref, m_ref, r_ref, z_ref, f_ref, acc_ref):
        m = m_ref[...]
        acc_ref[...] = jnp.zeros_like(acc_ref)
        for v in range(variables):
            x = jnp.concatenate([x_ref[slot, v] for slot in slots(SPREAD)], axis=0)
            s = jnp.dot(m, x, preferred_element_type=jnp.float32)
            for j in range(tiles):
                q = s[:, j * LANES : (j + 1) * LANES] * r_ref[j : j + 1, :]
                parts = {}
                for c in range(2):
                    for b in range(SEGMENT_NUMBER):
                        at = (c * SEGMENT_NUMBER + b) * modes
                        part = q[at : at + modes]
                        parts[c, b] = part
                        for k in range(own):
                            first = k * per_mode + (b * variables + v) * tiles * 2 + j * 2 + c
                            f_ref[pl.ds(first, groups, stride=height), :] = part[k * groups : (k + 1) * groups]
                r0, r1, i0, i1 = parts[0, 0], parts[0, 1], parts[1, 0], parts[1, 1]
                acc_ref[0:modes] += r0 * r0 + i0 * i0
                acc_ref[modes : 2 * modes] += r1 * r1 + i1 * i1
                acc_ref[2 * modes : 3 * modes] += r0 * r1 + i0 * i1
                acc_ref[3 * modes : 4 * modes] += r0 * i1 - i0 * r1
        total = lax.dot_general(
            jnp.ones((EXTRA, LANES), jnp.float32),
            acc_ref[...],
            (((1,), (1,)), ((), ())),
            precision=lax.Precision.HIGHEST,
            preferred_element_type=jnp.float32,
        )
        rounded = total.astype(jnp.bfloat16).astype(jnp.float32)
        row = lax.broadcasted_iota(jnp.int32, total.shape, 0)
        tail = jnp.where(row == 0, rounded, jnp.where(row == 1, total - rounded, 0.0))
        for d in range(groups):
            f_ref[d * height + own * per_mode : (d + 1) * height, :] = tail
        z_ref[...] = f_ref[...].reshape(z_ref.shape).astype(z_ref.dtype)

    vmem = pl.BlockSpec(memory_space=pltpu.VMEM)
    return pl.pallas_call(
        body,
        in_specs=[vmem, vmem, vmem],
        out_specs=vmem,
        out_shape=jax.ShapeDtypeStruct((groups, height, LANES), jnp.bfloat16),
        scratch_shapes=[
            pltpu.VMEM((groups * height, LANES), jnp.float32),
            pltpu.VMEM((4 * modes, LANES), jnp.float32),
        ],
        compiler_params=pltpu.CompilerParams(vmem_limit_bytes=VMEM_LIMIT),
        name="transform",
    )(gathered, multipliers, roots)


def unpack(received, rows, inner, copies):
    groups, _, lanes = received.shape
    outer = rows // inner

    def body(y_ref, o_ref, sums_ref):
        total = jnp.zeros((EXTRA, lanes), jnp.float32)
        for s, place in enumerate(slots(COLLECT)):
            piece = y_ref[place].astype(jnp.float32)
            o_ref[:, s * inner : (s + 1) * inner, :] = piece[:rows].reshape(outer, inner, lanes)
            total = total + piece[rows:]
        sums_ref[...] = jnp.broadcast_to((total[:1] + total[1:2])[None], sums_ref.shape)

    vmem = pl.BlockSpec(memory_space=pltpu.VMEM)
    return pl.pallas_call(
        body,
        in_specs=[vmem],
        out_specs=(vmem, vmem),
        out_shape=(
            pltpu.VMEM((outer, groups * inner, lanes), jnp.float32),
            pltpu.VMEM((copies, 1, lanes), jnp.float32),
        ),
        compiler_params=pltpu.CompilerParams(vmem_limit_bytes=VMEM_LIMIT),
        name="unpack",
    )(received)


def gram_of(sums, slot, groups, terms):
    own = RETAINED_MODES // groups
    entries = own * SEGMENT_NUMBER * SEGMENT_NUMBER
    lanes = sums.shape[-1]

    def body(slot_ref, sums_ref, gram_ref):
        total = sums_ref[0]
        for k in range(1, sums_ref.shape[0]):
            total = total + sums_ref[k]
        row = lax.broadcasted_iota(jnp.int32, (entries, lanes), 0)
        lane = lax.broadcasted_iota(jnp.int32, (entries, lanes), 1)
        f, b, b2 = row >> 2, (row >> 1) & 1, row & 1

        def chosen(q):
            there = lane == (q * own + f) * groups + slot_ref[0]
            return jnp.sum(jnp.where(there, total, 0.0), axis=1, keepdims=True) * jnp.float32(1.0 / terms)

        real = chosen(jnp.where(b == b2, b, 2))
        imag = chosen(3) * (b2 - b).astype(jnp.float32)
        both = jnp.where(lane == 0, real, imag)
        for k in range(entries // 2):
            gram_ref[k] = both[2 * k : 2 * k + 2, :2]

    vmem = pl.BlockSpec(memory_space=pltpu.VMEM)
    return pl.pallas_call(
        body,
        in_specs=[pl.BlockSpec(memory_space=pltpu.SMEM), vmem],
        out_specs=vmem,
        out_shape=jax.ShapeDtypeStruct((entries // 2, 2, 2), jnp.float32),
        compiler_params=pltpu.CompilerParams(vmem_limit_bytes=VMEM_LIMIT),
        name="gram",
    )(slot, sums)


def on_device(snapshots, quad_weights, spectral_indices):
    point_count = snapshots.shape[2]
    groups = lax.axis_size("ta")
    me = lax.axis_index("ta").astype(jnp.int32)
    own = RETAINED_MODES // groups
    tiles = point_count // groups // LANES
    rows = own * SEGMENT_NUMBER * VARS * tiles * 2

    weights = quad_weights.reshape(point_count // LANES, LANES)
    slot = slot_of(me, COLLECT)
    places = (me * groups + slot)[None]
    packed, multipliers, roots = pack(jnp.transpose(snapshots, (1, 0, 2)), spectral_indices, weights, places, groups)
    with jax.named_scope("spread"):
        gathered = exchange(packed, "ta", SPREAD)
    payload = transform(gathered, multipliers, roots)
    with jax.named_scope("collect"):
        received = exchange(payload, "ta", COLLECT)

    split = ("px", "py")
    copies = lax.axis_size(split)
    spectra, sums = unpack(received, rows, tiles * 2, copies)
    with jax.named_scope("points"):
        sums = exchange(sums, split, POINTS)
    gram = gram_of(sums, slot[None], groups, point_count * copies * VARS)
    gram = gram.reshape(own, SEGMENT_NUMBER, SEGMENT_NUMBER, 2)
    spectra = spectra.reshape(own, SEGMENT_NUMBER, VARS, point_count // LANES, 2, LANES)
    spectra = jnp.transpose(spectra, (0, 1, 4, 2, 3, 5)).reshape(own, SEGMENT_NUMBER, 2, VARS, point_count)
    return (spectra, gram)


def solution(mesh):
    return jax.shard_map(
        on_device,
        mesh=mesh,
        in_specs=(P("ta", None, ("px", "py")), P(("px", "py")), P()),
        out_specs=(P("ta", None, None, None, ("px", "py")), P("ta", None, None, None)),
        check_vma=False,
    )
```

```python
import math

import jax
import jax.numpy as jnp
from jax import lax
from jax.experimental import pallas as pl
from jax.experimental.pallas import tpu as pltpu
from jax.sharding import PartitionSpec as P

VARS = 5
BLK = 256
HOP = 128
SEGMENT_NUMBER = 2
RECORD_LENGTH = 384
RETAINED_MODES = 32
LANES = 128
VMEM_LIMIT = 16 << 20
EXTRA = 8
SPREAD = (11, 10, 4, 15, 12, 14, 8, 0, 7, 5, 1, 2, 13, 3, 9, 6)
COLLECT = (14, 7, 2, 11, 10, 13, 3, 15, 1, 9, 5, 0, 6, 12, 8, 4)
POINTS = (12, 0, 1, 2, 3, 4, 5, 6, 7, 8, 9, 10, 11, 13, 14, 15)


def slots(order):
    return [order.index(d) for d in range(len(order))]


def slot_of(device, order):
    words = [sum(slot << 4 * k for k, slot in enumerate(slots(order)[at : at + 7])) for at in (0, 7, 14)]
    word = jnp.where(device < 7, words[0], jnp.where(device < 14, words[1], words[2]))
    return lax.shift_right_logical(word, 4 * lax.rem(device, 7)) & 15


def exchange(pieces, axes, order):
    groups = [list(order)] if len(order) == pieces.shape[0] else None
    return lax.all_to_all(pieces, axes, split_axis=0, concat_axis=0, tiled=True, axis_index_groups=groups)


def cos_sin(turns):
    quarter = ((turns + 32) >> 6) & 3
    x = (((turns + 32) & 63) - 32).astype(jnp.float32) * jnp.float32(2.0 * math.pi / BLK)
    y = x * x
    cos = 1.0 + y * (-1 / 2 + y * (1 / 24 + y * (-1 / 720 + y * (1 / 40320 - y * (1 / 3628800)))))
    sin = x * (1.0 + y * (-1 / 6 + y * (1 / 120 + y * (-1 / 5040 + y * (1 / 362880)))))
    odd = (quarter & 1) == 1
    cos, sin = jnp.where(odd, sin, cos), jnp.where(odd, cos, sin)
    return jnp.where((quarter == 1) | (quarter == 2), -cos, cos), jnp.where(quarter >= 2, -sin, sin)


def multipliers_of(index_ref, own):
    modes = index_ref.shape[0]
    places = modes // own
    row = lax.broadcasted_iota(jnp.int32, (modes, BLK), 0)
    lag = lax.broadcasted_iota(jnp.int32, (modes, BLK), 1)
    index = jnp.zeros((modes, BLK), jnp.int32)
    for f in range(modes):
        index = jnp.where(row == f % own * places + slots(COLLECT)[f // own], index_ref[f], index)
    window = 0.5 - 0.5 * cos_sin(lax.broadcasted_iota(jnp.int32, (8, BLK), 1))[0]
    window = (window / jnp.sqrt(jnp.float32(3.0 * BLK / 8.0)))[:1]
    cos, sin = cos_sin((index * lag) & (BLK - 1))
    return cos * window, -sin * window


def pack(shard, indices, weights, places, groups):
    variables, times, points = shard.shape
    piece = points // groups
    modes = indices.shape[0]

    tiles = piece // LANES

    def body(places_ref, index_hbm, w_hbm, x_hbm, o_ref, m_ref, r_ref, index_ref, w_ref, x_ref, sem, index_sem, w_sem):
        get_index = pltpu.make_async_copy(index_hbm, index_ref, index_sem)
        get_weights = pltpu.make_async_copy(w_hbm, w_ref, w_sem)
        get_index.start()
        copies = [pltpu.make_async_copy(x_hbm.at[v], x_ref.at[v], sem.at[v]) for v in range(variables)]
        for copy in copies:
            copy.start()
        get_weights.start()
        m_ref[...] = jnp.zeros_like(m_ref)
        get_index.wait()
        for c, part in enumerate(multipliers_of(index_ref, modes // groups)):
            for b in range(SEGMENT_NUMBER):
                at = (c * SEGMENT_NUMBER + b) * modes
                m_ref[at : at + modes, b * HOP : b * HOP + BLK] = part.astype(m_ref.dtype)
        get_weights.wait()
        me = lax.div(places_ref[0], groups)
        r_ref[...] = jnp.sqrt(w_ref[pl.ds(me * tiles, tiles), :])
        for v, copy in enumerate(copies):
            copy.wait()
            for d, slot in enumerate(slots(SPREAD)):
                o_ref[slot, v] = x_ref[v, :, d * piece : (d + 1) * piece]

    vmem = pl.BlockSpec(memory_space=pltpu.VMEM)
    smem = pl.BlockSpec(memory_space=pltpu.SMEM)
    hbm = pl.BlockSpec(memory_space=pltpu.HBM)
    arrays = [pltpu.with_memory_space_constraint(array, pltpu.HBM) for array in (indices, weights, shard)]
    return pl.pallas_call(
        body,
        in_specs=[smem, hbm, hbm, hbm],
        out_specs=(vmem, vmem, vmem),
        out_shape=(
            jax.ShapeDtypeStruct((groups, variables, times, piece), shard.dtype),
            jax.ShapeDtypeStruct((2 * SEGMENT_NUMBER * modes, RECORD_LENGTH), jnp.bfloat16),
            jax.ShapeDtypeStruct((tiles, LANES), jnp.float32),
        ),
        scratch_shapes=[
            pltpu.SMEM(indices.shape, indices.dtype),
            pltpu.VMEM(weights.shape, weights.dtype),
            pltpu.VMEM(shard.shape, shard.dtype),
            pltpu.SemaphoreType.DMA((variables,)),
            pltpu.SemaphoreType.DMA,
            pltpu.SemaphoreType.DMA,
        ],
        compiler_params=pltpu.CompilerParams(vmem_limit_bytes=VMEM_LIMIT),
        name="pack",
    )(places, *arrays)


def transform(gathered, multipliers, roots):
    groups, variables, times, piece = gathered.shape
    tiles = piece // LANES
    modes = RETAINED_MODES
    own = modes // groups
    per_mode = SEGMENT_NUMBER * variables * tiles * 2
    height = own * per_mode + EXTRA

    def body(x_ref, m_ref, r_ref, z_ref, f_ref, acc_ref):
        m = m_ref[...]
        acc_ref[...] = jnp.zeros_like(acc_ref)
        for v in range(variables):
            x = jnp.concatenate([x_ref[slot, v] for slot in slots(SPREAD)], axis=0)
            s = jnp.dot(m, x, preferred_element_type=jnp.float32)
            for j in range(tiles):
                q = s[:, j * LANES : (j + 1) * LANES] * r_ref[j : j + 1, :]
                parts = {}
                for c in range(2):
                    for b in range(SEGMENT_NUMBER):
                        at = (c * SEGMENT_NUMBER + b) * modes
                        part = q[at : at + modes]
                        parts[c, b] = part
                        for k in range(own):
                            first = k * per_mode + (b * variables + v) * tiles * 2 + j * 2 + c
                            f_ref[pl.ds(first, groups, stride=height), :] = part[k * groups : (k + 1) * groups]
                r0, r1, i0, i1 = parts[0, 0], parts[0, 1], parts[1, 0], parts[1, 1]
                acc_ref[0:modes] += r0 * r0 + i0 * i0
                acc_ref[modes : 2 * modes] += r1 * r1 + i1 * i1
                acc_ref[2 * modes : 3 * modes] += r0 * r1 + i0 * i1
                acc_ref[3 * modes : 4 * modes] += r0 * i1 - i0 * r1
        total = lax.dot_general(
            jnp.ones((EXTRA, LANES), jnp.float32),
            acc_ref[...],
            (((1,), (1,)), ((), ())),
            precision=lax.Precision.HIGHEST,
            preferred_element_type=jnp.float32,
        )
        rounded = total.astype(jnp.bfloat16).astype(jnp.float32)
        row = lax.broadcasted_iota(jnp.int32, total.shape, 0)
        tail = jnp.where(row == 0, rounded, jnp.where(row == 1, total - rounded, 0.0))
        for d in range(groups):
            f_ref[d * height + own * per_mode : (d + 1) * height, :] = tail
        z_ref[...] = f_ref[...].reshape(z_ref.shape).astype(z_ref.dtype)

    vmem = pl.BlockSpec(memory_space=pltpu.VMEM)
    return pl.pallas_call(
        body,
        in_specs=[vmem, vmem, vmem],
        out_specs=vmem,
        out_shape=jax.ShapeDtypeStruct((groups, height, LANES), jnp.bfloat16),
        scratch_shapes=[
            pltpu.VMEM((groups * height, LANES), jnp.float32),
            pltpu.VMEM((4 * modes, LANES), jnp.float32),
        ],
        compiler_params=pltpu.CompilerParams(vmem_limit_bytes=VMEM_LIMIT),
        name="transform",
    )(gathered, multipliers, roots)


def unpack(received, rows, inner, copies):
    groups, _, lanes = received.shape
    outer = rows // inner

    def body(y_ref, o_ref, sums_hbm, sums_ref, sem):
        total = jnp.zeros((EXTRA, lanes), jnp.float32)
        for place in range(groups):
            total = total + y_ref[place, rows:, :].astype(jnp.float32)
        sums_ref[...] = jnp.broadcast_to((total[:1] + total[1:2])[None], sums_ref.shape)
        copy = pltpu.make_async_copy(sums_ref, sums_hbm, sem)
        copy.start()
        for s, place in enumerate(slots(COLLECT)):
            piece = y_ref[place, :rows, :].astype(jnp.float32)
            o_ref[:, s * inner : (s + 1) * inner, :] = piece.reshape(outer, inner, lanes)
        copy.wait()

    vmem = pl.BlockSpec(memory_space=pltpu.VMEM)
    return pl.pallas_call(
        body,
        in_specs=[vmem],
        out_specs=(vmem, pl.BlockSpec(memory_space=pltpu.HBM)),
        out_shape=(
            pltpu.VMEM((outer, groups * inner, lanes), jnp.float32),
            jax.ShapeDtypeStruct((copies, 1, lanes), jnp.float32),
        ),
        scratch_shapes=[pltpu.VMEM((copies, 1, lanes), jnp.float32), pltpu.SemaphoreType.DMA],
        compiler_params=pltpu.CompilerParams(vmem_limit_bytes=VMEM_LIMIT),
        name="unpack",
    )(received)


def gram_of(sums, slot, groups, terms):
    own = RETAINED_MODES // groups
    entries = own * SEGMENT_NUMBER * SEGMENT_NUMBER
    lanes = sums.shape[-1]

    def body(slot_ref, sums_ref, gram_ref):
        total = sums_ref[0]
        for k in range(1, sums_ref.shape[0]):
            total = total + sums_ref[k]
        row = lax.broadcasted_iota(jnp.int32, (entries, lanes), 0)
        lane = lax.broadcasted_iota(jnp.int32, (entries, lanes), 1)
        f, b, b2 = row >> 2, (row >> 1) & 1, row & 1

        def chosen(q):
            there = lane == (q * own + f) * groups + slot_ref[0]
            return jnp.sum(jnp.where(there, total, 0.0), axis=1, keepdims=True) * jnp.float32(1.0 / terms)

        real = chosen(jnp.where(b == b2, b, 2))
        imag = chosen(3) * (b2 - b).astype(jnp.float32)
        both = jnp.where(lane == 0, real, imag)
        for k in range(entries // 2):
            gram_ref[k] = both[2 * k : 2 * k + 2, :2]

    vmem = pl.BlockSpec(memory_space=pltpu.VMEM)
    return pl.pallas_call(
        body,
        in_specs=[pl.BlockSpec(memory_space=pltpu.SMEM), vmem],
        out_specs=vmem,
        out_shape=jax.ShapeDtypeStruct((entries // 2, 2, 2), jnp.float32),
        compiler_params=pltpu.CompilerParams(vmem_limit_bytes=VMEM_LIMIT),
        name="gram",
    )(slot, sums)


def on_device(snapshots, quad_weights, spectral_indices):
    point_count = snapshots.shape[2]
    groups = lax.axis_size("ta")
    me = lax.axis_index("ta").astype(jnp.int32)
    own = RETAINED_MODES // groups
    tiles = point_count // groups // LANES
    rows = own * SEGMENT_NUMBER * VARS * tiles * 2

    weights = quad_weights.reshape(point_count // LANES, LANES)
    slot = slot_of(me, COLLECT)
    places = (me * groups + slot)[None]
    packed, multipliers, roots = pack(jnp.transpose(snapshots, (1, 0, 2)), spectral_indices, weights, places, groups)
    with jax.named_scope("spread"):
        gathered = exchange(packed, "ta", SPREAD)
    payload = transform(gathered, multipliers, roots)
    with jax.named_scope("collect"):
        received = exchange(payload, "ta", COLLECT)

    split = ("px", "py")
    copies = lax.axis_size(split)
    spectra, sums = unpack(received, rows, tiles * 2, copies)
    with jax.named_scope("points"):
        sums = exchange(sums, split, POINTS)
    gram = gram_of(sums, slot[None], groups, point_count * copies * VARS)
    gram = gram.reshape(own, SEGMENT_NUMBER, SEGMENT_NUMBER, 2)
    spectra = spectra.reshape(own, SEGMENT_NUMBER, VARS, point_count // LANES, 2, LANES)
    spectra = jnp.transpose(spectra, (0, 1, 4, 2, 3, 5)).reshape(own, SEGMENT_NUMBER, 2, VARS, point_count)
    return (spectra, gram)


def solution(mesh):
    return jax.shard_map(
        on_device,
        mesh=mesh,
        in_specs=(P("ta", None, ("px", "py")), P(("px", "py")), P()),
        out_specs=(P("ta", None, None, None, ("px", "py")), P("ta", None, None, None)),
        check_vma=False,
    )
```
